32 devices in a mesh: gx: 4 (over y, x), gy: 8 (over z, core).
Axes of the slice: x: 2, y: 2, z: 4, core: 2. Of those that a mesh axis runs over, the one named last changes fastest.
Arguments:
- species_means: bfloat16 [8, 16, 120, 512], P(None, 'gy', None, 'gx'), may hold values from 0.19921875 to 5
- zonal_edge_velocity: float32 [16, 120, 512], P('gy', None, 'gx'), may hold values from -6 to 6
- meridional_edge_velocity: float32 [16, 120, 512], P('gy', None, 'gx'), may hold values from -6 to 6
- scaled_warmth: float32 [16, 120, 512], P('gy', None, 'gx'), may hold values from 0.5 to 2
- donor_depths: float32 [16, 120, 512], P('gy', None, 'gx'), may hold values from 0.5 to 2
- leading_donor_level: int32 [16, 120, 512], P('gy', None, 'gx'), may hold values from 0 to 118, as said below
- opening_share: bfloat16 [16, 120, 512], P('gy', None, 'gx'), may hold values from 0 to 0.44921875
- closing_share: bfloat16 [16, 120, 512], P('gy', None, 'gx'), may hold values from 0.546875 to 1
Outputs:
- tracers_out: float32 [8, 16, 120, 512], P(None, 'gy', None, 'gx')
- regridded_zonal: float32 [16, 120, 512], P('gy', None, 'gx')
- regridded_meridional: float32 [16, 120, 512], P('gy', None, 'gx')
- adjusted_warmth: float32 [16, 120, 512], P('gy', None, 'gx')
The draws below stay inside these ranges and needn't reach their ends.
Inputs may be any that keep to these rules, and one draw needn't show every extreme that they name: Target layer k draws on source layers leading_donor_level and leading_donor_level + 1, and leading_donor_level lies within 2 of k.
All inputs are finite; a program needn't handle non-finite values.
Results may differ from the reference program's by a relative error of at most 0.0003.
Values sent between devices are 32-bit elements; how exact they have to be, the bound alone decides.
A program may use at most 64 MiB of HBM per device.

```python
import math
import jax
import jax.numpy as jnp
from jax import lax

NTR = 8
LEVEL_NUMBER = 120
EASTWARD_CELLS = 512
NORTHWARD_CELLS = 16


def draw_leading_donor_level(key, part):
    offset = jax.random.randint(key, (NORTHWARD_CELLS, LEVEL_NUMBER, EASTWARD_CELLS), -2, 3, dtype=jnp.int32)
    layer_index = jnp.arange(LEVEL_NUMBER, dtype=jnp.int32)[None, :, None]
    return jnp.clip(layer_index + offset, 0, LEVEL_NUMBER - 2).astype(jnp.int32)


def steps_of(key, shape, cuts, least, largest):
    level = 1.0
    for position, shards_of in cuts:
        steps = jax.random.uniform(jax.random.fold_in(jax.random.fold_in(key, 6), position), (shards_of,), jnp.float32, least / len(cuts), largest / len(cuts))
        level = level * jnp.repeat(jnp.exp(steps), shape[position] // shards_of).reshape((-1,) + (1,) * (len(shape) - 1 - position))
    return level


def bell_draw(own_key, shape, width, limit, pieces=(), kind=jnp.bfloat16):
    values = jax.random.normal(own_key, shape, jnp.float32) * width
    if len(pieces) > 0:
        values = steps_of(own_key, shape, pieces, -0.22, 0.18) * values
    return jnp.clip(values, min=-limit, max=limit).astype(kind)


def setup_inputs(seed: int = 0) -> dict:
    arg_keys = jax.random.split(jax.random.key(seed), 9)
    return {
        "species_means": jnp.clip(jnp.exp(math.log(5.0) - 3.2227897 * jax.random.uniform(arg_keys[0], (NTR, NORTHWARD_CELLS, LEVEL_NUMBER, EASTWARD_CELLS), jnp.float32) ** steps_of(arg_keys[0], (NTR, NORTHWARD_CELLS, LEVEL_NUMBER, EASTWARD_CELLS), ((1, 8), (3, 4)), -0.2, 0.2)), 0.19921875, 5.0).astype(jnp.bfloat16),
        "zonal_edge_velocity": bell_draw(arg_keys[1], (NORTHWARD_CELLS, LEVEL_NUMBER, EASTWARD_CELLS), 1.0, 6.0, ((0, 8), (2, 4)), jnp.float32),
        "meridional_edge_velocity": bell_draw(arg_keys[2], (NORTHWARD_CELLS, LEVEL_NUMBER, EASTWARD_CELLS), 1.0, 6.0, ((0, 8), (2, 4)), jnp.float32),
        "scaled_warmth": jnp.clip(jnp.exp(math.log(2.0) - 1.3862944 * jax.random.uniform(arg_keys[3], (NORTHWARD_CELLS, LEVEL_NUMBER, EASTWARD_CELLS), jnp.float32) ** steps_of(arg_keys[3], (NORTHWARD_CELLS, LEVEL_NUMBER, EASTWARD_CELLS), ((0, 8), (2, 4)), -0.2, 0.2)), 0.5, 2.0),
        "donor_depths": jnp.clip(jnp.exp(math.log(2.0) - 1.3862944 * jax.random.uniform(arg_keys[4], (NORTHWARD_CELLS, LEVEL_NUMBER, EASTWARD_CELLS), jnp.float32) ** steps_of(arg_keys[4], (NORTHWARD_CELLS, LEVEL_NUMBER, EASTWARD_CELLS), ((0, 8), (2, 4)), -0.2, 0.2)), 0.5, 2.0),
        "leading_donor_level": draw_leading_donor_level(jax.random.fold_in(arg_keys[8], 71), 0),
        "opening_share": jnp.clip(0.44921875 * jax.random.uniform(arg_keys[6], (NORTHWARD_CELLS, LEVEL_NUMBER, EASTWARD_CELLS), jnp.float32) ** steps_of(arg_keys[6], (NORTHWARD_CELLS, LEVEL_NUMBER, EASTWARD_CELLS), ((0, 8), (2, 4)), -0.2, 0.2), 0.0, 0.44921875).astype(jnp.bfloat16),
        "closing_share": jnp.clip(0.546875 + 0.453125 * jax.random.uniform(arg_keys[7], (NORTHWARD_CELLS, LEVEL_NUMBER, EASTWARD_CELLS), jnp.float32) ** steps_of(arg_keys[7], (NORTHWARD_CELLS, LEVEL_NUMBER, EASTWARD_CELLS), ((0, 8), (2, 4)), -0.2, 0.2), 0.546875, 1.0).astype(jnp.bfloat16),
    }


thermal_rescale_factor = 3.5


def ppm_parts(values):
    layers = values.shape[-2]
    top_edge = 1.5 * values[..., 0:1, :] - 0.5 * values[..., 1:2, :]
    second_edge = 0.5 * (values[..., 0:1, :] + values[..., 1:2, :])
    inner_edge = (7.0 / 12.0) * (values[..., 1:layers - 2, :] + values[..., 2:layers - 1, :]) - (1.0 / 12.0) * (values[..., 0:layers - 3, :] + values[..., 3:layers, :])
    lower_edge = 0.5 * (values[..., layers - 2:layers - 1, :] + values[..., layers - 1:layers, :])
    bottom_edge = 1.5 * values[..., layers - 1:layers, :] - 0.5 * values[..., layers - 2:layers - 1, :]
    edge_values = jnp.concatenate([top_edge, second_edge, inner_edge, lower_edge, bottom_edge], axis=-2)
    left_edge = edge_values[..., :layers, :]
    right_edge = edge_values[..., 1:, :]
    return left_edge, right_edge - left_edge, 6.0 * values - 3.0 * (left_edge + right_edge)


def build_operator(donor_depths, leading_donor_level, opening_share, closing_share):
    start_frac = opening_share.astype(jnp.float32)
    end_frac = closing_share.astype(jnp.float32)
    next_layer = leading_donor_level + 1
    weight_first = (1.0 - start_frac) * jnp.take_along_axis(donor_depths, leading_donor_level, axis=-2)
    weight_second = end_frac * jnp.take_along_axis(donor_depths, next_layer, axis=-2)
    linear_first = 0.5 * (start_frac + 1.0)
    square_first = linear_first - (start_frac * start_frac + start_frac + 1.0) / 3.0
    linear_second = 0.5 * end_frac
    square_second = linear_second - end_frac * end_frac / 3.0
    return (leading_donor_level, next_layer, weight_first, weight_second, linear_first, square_first, linear_second, square_second)


def multiply_by_regrid_operator(operator, values):
    leading_donor_level, next_layer, weight_first, weight_second, linear_first, square_first, linear_second, square_second = operator
    left_edge, edge_slope, curvature = ppm_parts(values)
    first_index = jnp.broadcast_to(leading_donor_level, values.shape)
    second_index = jnp.broadcast_to(next_layer, values.shape)
    mean_first = jnp.take_along_axis(left_edge, first_index, axis=-2) + jnp.take_along_axis(edge_slope, first_index, axis=-2) * linear_first + jnp.take_along_axis(curvature, first_index, axis=-2) * square_first
    mean_second = jnp.take_along_axis(left_edge, second_index, axis=-2) + jnp.take_along_axis(edge_slope, second_index, axis=-2) * linear_second + jnp.take_along_axis(curvature, second_index, axis=-2) * square_second
    return (weight_first * mean_first + weight_second * mean_second) / (weight_first + weight_second)


def reference(species_means, zonal_edge_velocity, meridional_edge_velocity, scaled_warmth, donor_depths, leading_donor_level, opening_share, closing_share):
    vertical_regrid_operator = build_operator(donor_depths, leading_donor_level, opening_share, closing_share)
    north_op = build_operator(jnp.roll(donor_depths, -1, axis=0), jnp.roll(leading_donor_level, -1, axis=0), jnp.roll(opening_share, -1, axis=0), jnp.roll(closing_share, -1, axis=0))
    east_op = build_operator(jnp.roll(donor_depths, -1, axis=2), jnp.roll(leading_donor_level, -1, axis=2), jnp.roll(opening_share, -1, axis=2), jnp.roll(closing_share, -1, axis=2))
    regridded_depths = vertical_regrid_operator[2] + vertical_regrid_operator[3]
    tracer_new = lax.map(lambda tracer_field: multiply_by_regrid_operator(vertical_regrid_operator, tracer_field.astype(jnp.float32)), species_means)
    regridded_warmth = multiply_by_regrid_operator(vertical_regrid_operator, scaled_warmth)
    regridded_zonal = 0.5 * (multiply_by_regrid_operator(vertical_regrid_operator, zonal_edge_velocity) + multiply_by_regrid_operator(north_op, zonal_edge_velocity))
    regridded_meridional = 0.5 * (multiply_by_regrid_operator(vertical_regrid_operator, meridional_edge_velocity) + multiply_by_regrid_operator(east_op, meridional_edge_velocity))
    mass_before = lax.map(lambda tracer_field: jnp.sum(tracer_field.astype(jnp.float32) * donor_depths), species_means)
    mass_after = lax.map(lambda tracer_field: jnp.sum(tracer_field * regridded_depths), tracer_new)
    aggregate_regridded = jnp.sum(regridded_depths)
    preceding_zonal_aggregates = 0.5 * (donor_depths + jnp.roll(donor_depths, -1, axis=0))
    preceding_meridional_aggregates = 0.5 * (donor_depths + jnp.roll(donor_depths, -1, axis=2))
    zonal_edge_following = 0.5 * (regridded_depths + jnp.roll(regridded_depths, -1, axis=0))
    meridional_edge_following = 0.5 * (regridded_depths + jnp.roll(regridded_depths, -1, axis=2))
    preceding_enthalpy = thermal_rescale_factor * jnp.sum(donor_depths * scaled_warmth) + 0.5 * jnp.sum(preceding_zonal_aggregates * zonal_edge_velocity * zonal_edge_velocity) + 0.5 * jnp.sum(preceding_meridional_aggregates * meridional_edge_velocity * meridional_edge_velocity)
    kinetic_thermal_following = thermal_rescale_factor * jnp.sum(regridded_depths * regridded_warmth) + 0.5 * jnp.sum(zonal_edge_following * regridded_zonal * regridded_zonal) + 0.5 * jnp.sum(meridional_edge_following * regridded_meridional * regridded_meridional)
    tracers_out = tracer_new + ((mass_before - mass_after) / aggregate_regridded)[:, None, None, None]
    adjusted_warmth = regridded_warmth + (preceding_enthalpy - kinetic_thermal_following) / (thermal_rescale_factor * aggregate_regridded)
    return tracers_out, regridded_zonal, regridded_meridional, adjusted_warmth
```

```python
import functools

import jax
import jax.numpy as jnp
from jax import lax
from jax.experimental import pallas as pl
from jax.experimental.pallas import tpu as pltpu
from jax.sharding import PartitionSpec as P

MESH = pl.DeviceIdType.MESH
HEAT = 3.5
PAD = 8
F32 = jnp.float32
OFFSETS = (-2, -1, 0, 1, 2)


def choose(masks, options):
    keys = sorted(options)
    if len(keys) == len(OFFSETS):
        value = options[keys[-1]]
        keys = keys[:-1]
    else:
        value = jnp.zeros_like(options[keys[0]])
    for o in keys:
        value = jnp.where(masks[o], options[o], value)
    return value


def build_weights(depth_at, level, start, end, first_layer):
    layer = lax.broadcasted_iota(jnp.int32, level.shape, 0) + first_layer
    offset = level - layer
    masks = {o: offset == o for o in OFFSETS}
    depths = {o: depth_at(o) for o in range(-2, 4)}
    weight_first = (1.0 - start) * choose(masks, {o: depths[o] for o in OFFSETS})
    weight_second = end * choose(masks, {o: depths[o + 1] for o in OFFSETS})
    thick = weight_first + weight_second
    inverse = 1.0 / thick
    g1 = weight_first * inverse
    g2 = weight_second * inverse
    lin1 = 0.5 * (start + 1.0)
    sq1 = lin1 - (start * start + start + 1.0) * (1.0 / 3.0)
    lin2 = 0.5 * end
    sq2 = lin2 - end * end * (1.0 / 3.0)
    c_e0 = g1 * (1.0 - lin1 - 3.0 * sq1) * (1.0 / 12.0)
    c_e1 = (g1 * (lin1 - 3.0 * sq1) + g2 * (1.0 - lin2 - 3.0 * sq2)) * (1.0 / 12.0)
    c_e2 = g2 * (lin2 - 3.0 * sq2) * (1.0 / 12.0)
    taps = {
        -2: -c_e0,
        -1: 7.0 * c_e0 - c_e1,
        0: 7.0 * (c_e0 + c_e1) - c_e2 + 6.0 * (g1 * sq1),
        1: 7.0 * (c_e1 + c_e2) - c_e0 + 6.0 * (g2 * sq2),
        2: 7.0 * c_e2 - c_e1,
        3: -c_e2,
    }
    weights = {}
    for j in range(-4, 6):
        weights[j] = choose(masks, {o: taps[j - o] for o in OFFSETS if -2 <= j - o <= 3})
    return weights, thick


def remap(weights, load):
    terms = [weights[j] * load(j) for j in range(-4, 6)]
    while len(terms) > 1:
        terms = [
            terms[i] + terms[i + 1] if i + 1 < len(terms) else terms[i]
            for i in range(0, len(terms), 2)
        ]
    return terms[0]


def ghosts(near, second, third):
    return near + second - third, 12.0 * second - 4.0 * near - 7.0 * third


def pad_ends(buf, layers):
    row = lax.broadcasted_iota(jnp.int32, (PAD, buf.shape[-1]), 0)
    one, two = ghosts(
        buf[PAD : PAD + 1, :], buf[PAD + 1 : PAD + 2, :], buf[PAD + 2 : PAD + 3, :]
    )
    buf[0:PAD, :] = jnp.where(row == PAD - 1, one, jnp.where(row == PAD - 2, two, 0.0))
    last = PAD + layers
    one, two = ghosts(
        buf[last - 1 : last, :], buf[last - 2 : last - 1, :], buf[last - 3 : last - 2, :]
    )
    buf[last : last + PAD, :] = jnp.where(row == 0, one, jnp.where(row == 1, two, 0.0))


def main_kernel(
    nx,
    ny,
    q_hbm,
    u_hbm,
    v_hbm,
    w_hbm,
    d_hbm,
    l_hbm,
    a_hbm,
    b_hbm,
    tr_out,
    zonal_out,
    merid_out,
    warm_out,
    corr_out,
    q_raw,
    a_raw,
    b_raw,
    level,
    q_pad,
    u_pad,
    v_pad,
    vr_pad,
    vb_pad,
    w_pad,
    d_pad,
    a32,
    b32,
    thick_all,
    packed,
    n_depth,
    n_level,
    n_start,
    n_end,
    e_packed,
    sums,
    mine_x,
    mine_y,
    got_x,
    got_y,
    in_sem,
    send_sem,
    recv_sem,
    x_send,
    x_recv,
    y_send,
    y_recv,
):
    tracers, rows, layers, lanes = q_raw.shape
    gx = lax.axis_index("gx")
    gy = lax.axis_index("gy")
    body = pl.ds(PAD, layers)

    def x_peer(k):
        return {"gx": lax.rem(gx + k, nx)}

    def y_peer(k):
        return {"gy": lax.rem(gy + k, ny)}

    loads = [
        pltpu.make_async_copy(a_hbm, a_raw, in_sem.at[0]),
        pltpu.make_async_copy(b_hbm, b_raw, in_sem.at[1]),
        pltpu.make_async_copy(l_hbm, level, in_sem.at[2]),
        pltpu.make_async_copy(d_hbm, d_pad.at[:, body, :], in_sem.at[3]),
        pltpu.make_async_copy(v_hbm, v_pad.at[:, body, :], in_sem.at[4]),
        pltpu.make_async_copy(u_hbm, u_pad.at[:, body, :], in_sem.at[5]),
        pltpu.make_async_copy(w_hbm, w_pad.at[:, body, :], in_sem.at[6]),
        pltpu.make_async_copy(q_hbm, q_raw, in_sem.at[7]),
    ]
    for load in loads:
        load.start()

    barrier = pltpu.get_barrier_semaphore()
    for k in range(1, nx):
        pl.semaphore_signal(barrier, inc=1, device_id=x_peer(k), device_id_type=MESH)
    for k in range(1, ny):
        pl.semaphore_signal(barrier, inc=1, device_id=y_peer(k), device_id_type=MESH)

    for load in loads[:4]:
        load.wait()
    lane_full = lax.broadcasted_iota(jnp.int32, (layers, lanes), 1)
    for r in range(rows):
        a32[r] = a_raw[r].astype(F32)
        b32[r] = b_raw[r].astype(F32)
    column = jnp.zeros((layers, lanes), F32)
    for r in range(rows):
        parts = (d_pad[r, PAD : PAD + layers, :], level[r].astype(F32), a32[r], b32[r])
        for q, part in enumerate(parts):
            spot = q * rows + r
            moved = pltpu.roll(part, spot, 1) if spot else part
            column = jnp.where(lane_full == spot, moved, column)
    packed[...] = column

    pl.semaphore_wait(barrier, nx + ny - 2)
    pairs = [
        (packed, e_packed.at[body, :], x_peer(nx - 1)),
        (d_pad.at[0, body, :], n_depth.at[body, :], y_peer(ny - 1)),
        (level.at[0], n_level, y_peer(ny - 1)),
        (a32.at[0], n_start, y_peer(ny - 1)),
        (b32.at[0], n_end, y_peer(ny - 1)),
    ]
    sends = [
        pltpu.make_async_remote_copy(
            src_ref=src,
            dst_ref=dst,
            send_sem=send_sem.at[i],
            recv_sem=recv_sem.at[i],
            device_id=peer,
            device_id_type=MESH,
        )
        for i, (src, dst, peer) in enumerate(pairs)
    ]
    for send in sends:
        send.start()

    for load in loads[4:7]:
        load.wait()
    for r in range(rows):
        d_pad[r, 0:PAD, :] = jnp.zeros((PAD, lanes), F32)
        d_pad[r, PAD + layers : PAD + layers + PAD, :] = jnp.zeros((PAD, lanes), F32)
        pad_ends(v_pad.at[r], layers)
        pad_ends(u_pad.at[r], layers)
        pad_ends(w_pad.at[r], layers)
    lane_tall = lax.broadcasted_iota(jnp.int32, (layers + 2 * PAD, lanes), 1)
    last_faces = jnp.zeros((layers + 2 * PAD, lanes), F32)
    for r in range(rows):
        wind = v_pad[r]
        turned = pltpu.roll(wind, 1, 1)
        vr_pad[r] = turned
        moved = pltpu.roll(turned, r, 1) if r else turned
        last_faces = jnp.where(lane_tall == r, moved, last_faces)
    vb_pad[...] = last_faces
    loads[7].wait()
    for t in range(tracers):
        for r in range(rows):
            q_pad[t, r, PAD : PAD + layers, :] = q_raw[t, r].astype(F32)
            pad_ends(q_pad.at[t, r], layers)

    lane = lax.broadcasted_iota(jnp.int32, (8, lanes), 1)
    not_first = lane > 0
    not_last = lane < lanes - 1
    zero = jnp.zeros((8, lanes), F32)

    def tile_step(i, carry):
        masses, total, energy = carry
        masses = list(masses)
        k0 = pl.multiple_of(i * 8, 8)
        here = pl.ds(k0, 8)

        def at(ref, j):
            return ref[pl.ds(k0 + (PAD + j), 8), :]

        own_before = None
        thick_before = None
        for r in range(rows):
            weights, thick = build_weights(
                lambda o: at(d_pad.at[r], o), level[r, here, :], a32[r, here, :], b32[r, here, :], k0
            )
            depth = at(d_pad.at[r], 0)
            thick_all[r, here, :] = thick
            total = total + thick
            for t in range(tracers):
                new = remap(weights, lambda j: at(q_pad.at[t, r], j))
                tr_out[t, r, here, :] = new
                masses[t] = masses[t] + (depth * at(q_pad.at[t, r], 0) - thick * new)
            warm = remap(weights, lambda j: at(w_pad.at[r], j))
            warm_out[r, here, :] = warm
            energy = energy + HEAT * (depth * at(w_pad.at[r], 0) - thick * warm)
            u_here = at(u_pad.at[r], 0)
            squares = u_here * u_here
            own = remap(weights, lambda j: at(u_pad.at[r], j))
            after = zero
            if r > 0:
                u_back = at(u_pad.at[r - 1], 0)
                squares = squares + u_back * u_back
                cross = remap(weights, lambda j: at(u_pad.at[r - 1], j))
                zonal = 0.5 * (own_before + cross)
                zonal_out[r - 1, here, :] = zonal
                after = (thick_before + thick) * (zonal * zonal)
            own_before = own
            thick_before = thick
            v_here = at(v_pad.at[r], 0)
            v_west = at(vr_pad.at[r], 0)
            squares = squares + v_here * v_here + jnp.where(not_first, v_west * v_west, 0.0)
            own_v = remap(weights, lambda j: at(v_pad.at[r], j))
            cross_v = remap(weights, lambda j: at(vr_pad.at[r], j))
            east_v = jnp.where(not_last, pltpu.roll(cross_v, lanes - 1, 1), 0.0)
            east_thick = pltpu.roll(thick, lanes - 1, 1)
            merid = 0.5 * (own_v + east_v)
            merid_out[r, here, :] = merid
            after = after + jnp.where(not_last, (thick + east_thick) * (merid * merid), 0.0)
            energy = energy + 0.25 * (depth * squares - after)
        zonal_out[rows - 1, here, :] = own_before
        return tuple(masses), total, energy

    masses, total, energy = lax.fori_loop(
        0, layers // 8, tile_step, ((zero,) * tracers, zero, zero)
    )
    sums[...] = jnp.zeros(sums.shape, F32)
    for t in range(tracers):
        sums[t : t + 1, :] = jnp.sum(masses[t], axis=0, keepdims=True)
    sums[tracers : tracers + 1, :] = jnp.sum(total, axis=0, keepdims=True)

    for send in sends:
        send.wait_recv()

    def edge_step(i, energy):
        k0 = pl.multiple_of(i * 8, 8)
        here = pl.ds(k0, 8)

        def at(ref, j):
            return ref[pl.ds(k0 + (PAD + j), 8), :]

        weights, thick = build_weights(
            lambda o: at(n_depth, o), n_level[here, :], n_start[here, :], n_end[here, :], k0
        )
        u_last = at(u_pad.at[rows - 1], 0)
        cross = remap(weights, lambda j: at(u_pad.at[rows - 1], j))
        zonal = 0.5 * (zonal_out[rows - 1, here, :] + cross)
        zonal_out[rows - 1, here, :] = zonal
        change = at(n_depth, 0) * (u_last * u_last) - (
            thick_all[rows - 1, here, :] + thick
        ) * (zonal * zonal)

        column = at(e_packed, 0)
        weights, thick = build_weights(
            lambda o: at(e_packed, o),
            pltpu.roll(column, lanes - rows, 1).astype(jnp.int32),
            pltpu.roll(column, lanes - 2 * rows, 1),
            pltpu.roll(column, lanes - 3 * rows, 1),
            k0,
        )
        cross = remap(weights, lambda j: at(vb_pad, j))
        face = at(vb_pad, 0)
        change = change + jnp.where(lane < rows, column * (face * face), 0.0)
        for r in range(rows):
            there = pltpu.roll(cross, lanes - 1 - r, 1)
            there_thick = pltpu.roll(thick, lanes - 1 - r, 1)
            merid = merid_out[r, here, :] + jnp.where(not_last, 0.0, 0.5 * there)
            merid_out[r, here, :] = merid
            change = change - jnp.where(
                not_last, 0.0, (thick_all[r, here, :] + there_thick) * (merid * merid)
            )
        return energy + 0.25 * change

    energy = lax.fori_loop(0, layers // 8, edge_step, energy)
    sums[tracers + 1 : tracers + 2, :] = jnp.sum(energy, axis=0, keepdims=True)

    wide = sums.shape
    diagonal = lax.broadcasted_iota(jnp.int32, wide, 0) == lax.broadcasted_iota(jnp.int32, wide, 1)
    column = jnp.sum(sums[...], axis=1, keepdims=True)
    mine_x[...] = jnp.sum(jnp.where(diagonal, column, 0.0), axis=0, keepdims=True)

    def gather(count, peer, mine, got, s_sem, r_sem):
        copies = [
            pltpu.make_async_remote_copy(
                src_ref=mine,
                dst_ref=got.at[k - 1],
                send_sem=s_sem.at[k - 1],
                recv_sem=r_sem.at[k - 1],
                device_id=peer(k),
                device_id_type=MESH,
            )
            for k in range(1, count)
        ]
        for copy in copies:
            copy.start()
        for copy in copies:
            copy.wait_recv()
        value = mine[...]
        for k in range(count - 1):
            value = value + got[k]
        return value, copies

    value, first_copies = gather(nx, x_peer, mine_x, got_x, x_send, x_recv)
    mine_y[...] = value
    value, second_copies = gather(ny, y_peer, mine_y, got_y, y_send, y_recv)

    spread = jnp.sum(jnp.where(diagonal, value, 0.0), axis=1, keepdims=True)
    total_new = spread[tracers : tracers + 1, :]
    change = spread / total_new
    index = lax.broadcasted_iota(jnp.int32, change.shape, 0)
    change = jnp.where(index == tracers + 1, change * (1.0 / HEAT), change)
    corr_out[...] = jnp.broadcast_to(change, corr_out.shape)
    for send in sends:
        send.wait_send()
    for copy in first_copies + second_copies:
        copy.wait_send()


def finish_kernel(
    tr,
    zonal,
    merid,
    warm,
    corr,
    tr_hbm,
    zonal_hbm,
    merid_hbm,
    warm_hbm,
    tr_buf,
    warm_buf,
    sem,
):
    tracers = tr.shape[0]
    copies = [
        pltpu.make_async_copy(zonal, zonal_hbm, sem.at[tracers]),
        pltpu.make_async_copy(merid, merid_hbm, sem.at[tracers + 1]),
    ]
    for copy in copies:
        copy.start()
    for t in range(tracers):
        tr_buf[t] = tr[t] + corr[t : t + 1, :][None]
        copy = pltpu.make_async_copy(tr_buf.at[t], tr_hbm.at[t], sem.at[t])
        copy.start()
        copies.append(copy)
    warm_buf[...] = warm[...] + corr[tracers + 1 : tracers + 2, :][None]
    copy = pltpu.make_async_copy(warm_buf, warm_hbm, sem.at[tracers + 2])
    copy.start()
    copies.append(copy)
    for copy in copies:
        copy.wait()


def local(nx, ny, q, u, v, w, d, level, a, b):
    tracers, rows, layers, lanes = q.shape
    tall = layers + 2 * PAD
    plane = (rows, layers, lanes)
    sum_rows = -(-(tracers + 2) // 8) * 8
    vmem = pltpu.VMEM
    dma = pltpu.SemaphoreType.DMA
    anywhere = pl.BlockSpec(memory_space=pl.ANY)
    inside = pl.BlockSpec(memory_space=vmem)
    middle = pl.pallas_call(
        functools.partial(main_kernel, nx, ny),
        name="remap_main",
        out_shape=[
            vmem((tracers,) + plane, F32),
            vmem(plane, F32),
            vmem(plane, F32),
            vmem(plane, F32),
            vmem((sum_rows, lanes), F32),
        ],
        in_specs=[anywhere] * 8,
        out_specs=[inside] * 5,
        scratch_shapes=[
            vmem((tracers,) + plane, jnp.bfloat16),
            vmem(plane, jnp.bfloat16),
            vmem(plane, jnp.bfloat16),
            vmem(plane, jnp.int32),
            vmem((tracers, rows, tall, lanes), F32),
            vmem((rows, tall, lanes), F32),
            vmem((rows, tall, lanes), F32),
            vmem((rows, tall, lanes), F32),
            vmem((tall, lanes), F32),
            vmem((rows, tall, lanes), F32),
            vmem((rows, tall, lanes), F32),
            vmem(plane, F32),
            vmem(plane, F32),
            vmem(plane, F32),
            vmem((layers, lanes), F32),
            vmem((tall, lanes), F32),
            vmem((layers, lanes), jnp.int32),
            vmem((layers, lanes), F32),
            vmem((layers, lanes), F32),
            vmem((tall, lanes), F32),
            vmem((sum_rows, lanes), F32),
            vmem((1, lanes), F32),
            vmem((1, lanes), F32),
            vmem((nx - 1, 1, lanes), F32),
            vmem((ny - 1, 1, lanes), F32),
            dma((8,)),
            dma((5,)),
            dma((5,)),
            dma((nx - 1,)),
            dma((nx - 1,)),
            dma((ny - 1,)),
            dma((ny - 1,)),
        ],
        compiler_params=pltpu.CompilerParams(collective_id=0, has_side_effects=True),
    )(q, u, v, w, d, level, a, b)
    return tuple(
        pl.pallas_call(
            finish_kernel,
            name="remap_finish",
            out_shape=[
                jax.ShapeDtypeStruct((tracers,) + plane, F32),
                jax.ShapeDtypeStruct(plane, F32),
                jax.ShapeDtypeStruct(plane, F32),
                jax.ShapeDtypeStruct(plane, F32),
            ],
            in_specs=[inside] * 5,
            out_specs=[anywhere] * 4,
            scratch_shapes=[
                vmem((tracers,) + plane, F32),
                vmem(plane, F32),
                dma((tracers + 3,)),
            ],
        )(*middle)
    )


def solution(mesh):
    flat = P("gy", None, "gx")
    tall = P(None, "gy", None, "gx")
    return jax.shard_map(
        functools.partial(local, mesh.shape["gx"], mesh.shape["gy"]),
        mesh=mesh,
        in_specs=(tall,) + (flat,) * 7,
        out_specs=(tall,) + (flat,) * 3,
        check_vma=False,
    )
```

```python
import functools

import jax
import jax.numpy as jnp
from jax import lax
from jax.experimental import pallas as pl
from jax.experimental.pallas import tpu as pltpu
from jax.sharding import PartitionSpec as P

MESH = pl.DeviceIdType.MESH
HEAT = 3.5
PAD = 8
F32 = jnp.float32
OFFSETS = (-2, -1, 0, 1, 2)


def choose(masks, options):
    keys = sorted(options)
    if len(keys) == len(OFFSETS):
        value = options[keys[-1]]
        keys = keys[:-1]
    else:
        value = jnp.zeros_like(options[keys[0]])
    for o in keys:
        value = jnp.where(masks[o], options[o], value)
    return value


def build_weights(depth_at, level, start, end, first_layer):
    layer = lax.broadcasted_iota(jnp.int32, level.shape, 0) + first_layer
    offset = level - layer
    masks = {o: offset == o for o in OFFSETS}
    depths = {o: depth_at(o) for o in range(-2, 4)}
    weight_first = (1.0 - start) * choose(masks, {o: depths[o] for o in OFFSETS})
    weight_second = end * choose(masks, {o: depths[o + 1] for o in OFFSETS})
    thick = weight_first + weight_second
    inverse = 1.0 / thick
    g1 = weight_first * inverse
    g2 = weight_second * inverse
    lin1 = 0.5 * (start + 1.0)
    sq1 = lin1 - (start * start + start + 1.0) * (1.0 / 3.0)
    lin2 = 0.5 * end
    sq2 = lin2 - end * end * (1.0 / 3.0)
    c_e0 = g1 * (1.0 - lin1 - 3.0 * sq1) * (1.0 / 12.0)
    c_e1 = (g1 * (lin1 - 3.0 * sq1) + g2 * (1.0 - lin2 - 3.0 * sq2)) * (1.0 / 12.0)
    c_e2 = g2 * (lin2 - 3.0 * sq2) * (1.0 / 12.0)
    taps = {
        -2: -c_e0,
        -1: 7.0 * c_e0 - c_e1,
        0: 7.0 * (c_e0 + c_e1) - c_e2 + 6.0 * (g1 * sq1),
        1: 7.0 * (c_e1 + c_e2) - c_e0 + 6.0 * (g2 * sq2),
        2: 7.0 * c_e2 - c_e1,
        3: -c_e2,
    }
    weights = {}
    for j in range(-4, 6):
        weights[j] = choose(masks, {o: taps[j - o] for o in OFFSETS if -2 <= j - o <= 3})
    return weights, thick


def remap(weights, load):
    terms = [weights[j] * load(j) for j in range(-4, 6)]
    while len(terms) > 1:
        terms = [
            terms[i] + terms[i + 1] if i + 1 < len(terms) else terms[i]
            for i in range(0, len(terms), 2)
        ]
    return terms[0]


def ghosts(near, second, third):
    return near + second - third, 12.0 * second - 4.0 * near - 7.0 * third


def pad_ends(buf, layers):
    row = lax.broadcasted_iota(jnp.int32, (PAD, buf.shape[-1]), 0)
    one, two = ghosts(
        buf[PAD : PAD + 1, :], buf[PAD + 1 : PAD + 2, :], buf[PAD + 2 : PAD + 3, :]
    )
    buf[0:PAD, :] = jnp.where(row == PAD - 1, one, jnp.where(row == PAD - 2, two, 0.0))
    last = PAD + layers
    one, two = ghosts(
        buf[last - 1 : last, :], buf[last - 2 : last - 1, :], buf[last - 3 : last - 2, :]
    )
    buf[last : last + PAD, :] = jnp.where(row == 0, one, jnp.where(row == 1, two, 0.0))


def main_kernel(
    nx,
    ny,
    q_hbm,
    u_hbm,
    v_hbm,
    w_hbm,
    d_hbm,
    l_hbm,
    a_hbm,
    b_hbm,
    tr_out,
    zonal_out,
    merid_out,
    warm_out,
    corr_out,
    q_raw,
    a_raw,
    b_raw,
    level,
    q_pad,
    u_pad,
    v_pad,
    vr_pad,
    vb_pad,
    w_pad,
    d_pad,
    a32,
    b32,
    thick_all,
    packed,
    n_depth,
    n_level,
    n_start,
    n_end,
    e_packed,
    sums,
    mine_x,
    mine_y,
    got_x,
    got_y,
    in_sem,
    send_sem,
    recv_sem,
    x_send,
    x_recv,
    y_send,
    y_recv,
):
    tracers, rows, layers, lanes = q_raw.shape
    gx = lax.axis_index("gx")
    gy = lax.axis_index("gy")
    body = pl.ds(PAD, layers)

    def x_peer(k):
        return {"gx": lax.rem(gx + k, nx)}

    def y_peer(k):
        return {"gy": lax.rem(gy + k, ny)}

    loads = [
        pltpu.make_async_copy(a_hbm, a_raw, in_sem.at[0]),
        pltpu.make_async_copy(b_hbm, b_raw, in_sem.at[1]),
        pltpu.make_async_copy(l_hbm, level, in_sem.at[2]),
        pltpu.make_async_copy(d_hbm, d_pad.at[:, body, :], in_sem.at[3]),
        pltpu.make_async_copy(v_hbm, v_pad.at[:, body, :], in_sem.at[4]),
        pltpu.make_async_copy(u_hbm, u_pad.at[:, body, :], in_sem.at[5]),
        pltpu.make_async_copy(w_hbm, w_pad.at[:, body, :], in_sem.at[6]),
        pltpu.make_async_copy(q_hbm, q_raw, in_sem.at[7]),
    ]
    for load in loads:
        load.start()

    barrier = pltpu.get_barrier_semaphore()
    for k in range(1, nx):
        pl.semaphore_signal(barrier, inc=1, device_id=x_peer(k), device_id_type=MESH)
    for k in range(1, ny):
        pl.semaphore_signal(barrier, inc=1, device_id=y_peer(k), device_id_type=MESH)

    for load in loads[:4]:
        load.wait()
    lane_full = lax.broadcasted_iota(jnp.int32, (layers, lanes), 1)
    for r in range(rows):
        a32[r] = a_raw[r].astype(F32)
        b32[r] = b_raw[r].astype(F32)
    column = jnp.zeros((layers, lanes), F32)
    for r in range(rows):
        parts = (d_pad[r, PAD : PAD + layers, :], level[r].astype(F32), a32[r], b32[r])
        for q, part in enumerate(parts):
            spot = q * rows + r
            moved = pltpu.roll(part, spot, 1) if spot else part
            column = jnp.where(lane_full == spot, moved, column)
    packed[...] = column

    pl.semaphore_wait(barrier, nx + ny - 2)
    pairs = [
        (packed, e_packed.at[body, :], x_peer(nx - 1)),
        (d_pad.at[0, body, :], n_depth.at[body, :], y_peer(ny - 1)),
        (level.at[0], n_level, y_peer(ny - 1)),
        (a32.at[0], n_start, y_peer(ny - 1)),
        (b32.at[0], n_end, y_peer(ny - 1)),
    ]
    sends = [
        pltpu.make_async_remote_copy(
            src_ref=src,
            dst_ref=dst,
            send_sem=send_sem.at[i],
            recv_sem=recv_sem.at[i],
            device_id=peer,
            device_id_type=MESH,
        )
        for i, (src, dst, peer) in enumerate(pairs)
    ]
    for send in sends:
        send.start()

    for load in loads[4:7]:
        load.wait()
    for r in range(rows):
        d_pad[r, 0:PAD, :] = jnp.zeros((PAD, lanes), F32)
        d_pad[r, PAD + layers : PAD + layers + PAD, :] = jnp.zeros((PAD, lanes), F32)
        pad_ends(v_pad.at[r], layers)
        pad_ends(u_pad.at[r], layers)
        pad_ends(w_pad.at[r], layers)
    lane_tall = lax.broadcasted_iota(jnp.int32, (layers + 2 * PAD, lanes), 1)
    last_faces = jnp.zeros((layers + 2 * PAD, lanes), F32)
    for r in range(rows):
        wind = v_pad[r]
        turned = pltpu.roll(wind, 1, 1)
        vr_pad[r] = turned
        moved = pltpu.roll(turned, r, 1) if r else turned
        last_faces = jnp.where(lane_tall == r, moved, last_faces)
    vb_pad[...] = last_faces
    loads[7].wait()
    for t in range(tracers):
        for r in range(rows):
            q_pad[t, r, PAD : PAD + layers, :] = q_raw[t, r].astype(F32)
            pad_ends(q_pad.at[t, r], layers)

    lane = lax.broadcasted_iota(jnp.int32, (8, lanes), 1)
    not_first = lane > 0
    not_last = lane < lanes - 1
    zero = jnp.zeros((8, lanes), F32)

    def tile_step(i, carry):
        masses, total, energy = carry
        masses = list(masses)
        k0 = pl.multiple_of(i * 8, 8)
        here = pl.ds(k0, 8)

        def at(ref, j):
            return ref[pl.ds(k0 + (PAD + j), 8), :]

        own_before = None
        thick_before = None
        for r in range(rows):
            weights, thick = build_weights(
                lambda o: at(d_pad.at[r], o), level[r, here, :], a32[r, here, :], b32[r, here, :], k0
            )
            depth = at(d_pad.at[r], 0)
            thick_all[r, here, :] = thick
            total = total + thick
            for t in range(tracers):
                new = remap(weights, lambda j: at(q_pad.at[t, r], j))
                tr_out[t, r, here, :] = new
                masses[t] = masses[t] + (depth * at(q_pad.at[t, r], 0) - thick * new)
            warm = remap(weights, lambda j: at(w_pad.at[r], j))
            warm_out[r, here, :] = warm
            energy = energy + HEAT * (depth * at(w_pad.at[r], 0) - thick * warm)
            u_here = at(u_pad.at[r], 0)
            squares = u_here * u_here
            own = remap(weights, lambda j: at(u_pad.at[r], j))
            after = zero
            if r > 0:
                u_back = at(u_pad.at[r - 1], 0)
                squares = squares + u_back * u_back
                cross = remap(weights, lambda j: at(u_pad.at[r - 1], j))
                zonal = 0.5 * (own_before + cross)
                zonal_out[r - 1, here, :] = zonal
                after = (thick_before + thick) * (zonal * zonal)
            own_before = own
            thick_before = thick
            v_here = at(v_pad.at[r], 0)
            v_west = at(vr_pad.at[r], 0)
            squares = squares + v_here * v_here + jnp.where(not_first, v_west * v_west, 0.0)
            own_v = remap(weights, lambda j: at(v_pad.at[r], j))
            cross_v = remap(weights, lambda j: at(vr_pad.at[r], j))
            east_v = jnp.where(not_last, pltpu.roll(cross_v, lanes - 1, 1), 0.0)
            east_thick = pltpu.roll(thick, lanes - 1, 1)
            merid = 0.5 * (own_v + east_v)
            merid_out[r, here, :] = merid
            after = after + jnp.where(not_last, (thick + east_thick) * (merid * merid), 0.0)
            energy = energy + 0.25 * (depth * squares - after)
        zonal_out[rows - 1, here, :] = own_before
        return tuple(masses), total, energy

    masses, total, energy = lax.fori_loop(
        0, layers // 8, tile_step, ((zero,) * tracers, zero, zero)
    )
    sums[...] = jnp.zeros(sums.shape, F32)
    for t in range(tracers):
        sums[t : t + 1, :] = jnp.sum(masses[t], axis=0, keepdims=True)
    sums[tracers : tracers + 1, :] = jnp.sum(total, axis=0, keepdims=True)

    for send in sends:
        send.wait_recv()

    def edge_step(i, energy):
        k0 = pl.multiple_of(i * 8, 8)
        here = pl.ds(k0, 8)

        def at(ref, j):
            return ref[pl.ds(k0 + (PAD + j), 8), :]

        weights, thick = build_weights(
            lambda o: at(n_depth, o), n_level[here, :], n_start[here, :], n_end[here, :], k0
        )
        u_last = at(u_pad.at[rows - 1], 0)
        cross = remap(weights, lambda j: at(u_pad.at[rows - 1], j))
        zonal = 0.5 * (zonal_out[rows - 1, here, :] + cross)
        zonal_out[rows - 1, here, :] = zonal
        change = at(n_depth, 0) * (u_last * u_last) - (
            thick_all[rows - 1, here, :] + thick
        ) * (zonal * zonal)

        column = at(e_packed, 0)
        weights, thick = build_weights(
            lambda o: at(e_packed, o),
            pltpu.roll(column, lanes - rows, 1).astype(jnp.int32),
            pltpu.roll(column, lanes - 2 * rows, 1),
            pltpu.roll(column, lanes - 3 * rows, 1),
            k0,
        )
        cross = remap(weights, lambda j: at(vb_pad, j))
        face = at(vb_pad, 0)
        change = change + jnp.where(lane < rows, column * (face * face), 0.0)
        for r in range(rows):
            there = pltpu.roll(cross, lanes - 1 - r, 1)
            there_thick = pltpu.roll(thick, lanes - 1 - r, 1)
            merid = merid_out[r, here, :] + jnp.where(not_last, 0.0, 0.5 * there)
            merid_out[r, here, :] = merid
            change = change - jnp.where(
                not_last, 0.0, (thick_all[r, here, :] + there_thick) * (merid * merid)
            )
        return energy + 0.25 * change

    energy = lax.fori_loop(0, layers // 8, edge_step, energy)
    sums[tracers + 1 : tracers + 2, :] = jnp.sum(energy, axis=0, keepdims=True)

    wide = sums.shape
    diagonal = lax.broadcasted_iota(jnp.int32, wide, 0) == lax.broadcasted_iota(jnp.int32, wide, 1)
    column = jnp.sum(sums[...], axis=1, keepdims=True)
    mine_x[...] = jnp.sum(jnp.where(diagonal, column, 0.0), axis=0, keepdims=True)

    def gather(count, peer, mine, got, s_sem, r_sem):
        copies = [
            pltpu.make_async_remote_copy(
                src_ref=mine,
                dst_ref=got.at[k - 1],
                send_sem=s_sem.at[k - 1],
                recv_sem=r_sem.at[k - 1],
                device_id=peer(k),
                device_id_type=MESH,
            )
            for k in range(1, count)
        ]
        for copy in copies:
            copy.start()
        for copy in copies:
            copy.wait_recv()
        value = mine[...]
        for k in range(count - 1):
            value = value + got[k]
        return value, copies

    value, first_copies = gather(nx, x_peer, mine_x, got_x, x_send, x_recv)
    mine_y[...] = value
    value, second_copies = gather(ny, y_peer, mine_y, got_y, y_send, y_recv)

    spread = jnp.sum(jnp.where(diagonal, value, 0.0), axis=1, keepdims=True)
    total_new = spread[tracers : tracers + 1, :]
    change = spread / total_new
    index = lax.broadcasted_iota(jnp.int32, change.shape, 0)
    change = jnp.where(index == tracers + 1, change * (1.0 / HEAT), change)
    corr_out[...] = jnp.broadcast_to(change, corr_out.shape)
    for send in sends:
        send.wait_send()
    for copy in first_copies + second_copies:
        copy.wait_send()


def finish_kernel(
    tr,
    zonal,
    merid,
    warm,
    corr,
    tr_hbm,
    zonal_hbm,
    merid_hbm,
    warm_hbm,
    tr_buf,
    warm_buf,
    sem,
):
    tracers = tr.shape[0]
    copies = [
        pltpu.make_async_copy(zonal, zonal_hbm, sem.at[tracers]),
        pltpu.make_async_copy(merid, merid_hbm, sem.at[tracers + 1]),
    ]
    for copy in copies:
        copy.start()
    for t in range(tracers):
        tr_buf[t] = tr[t] + corr[t : t + 1, :][None]
        copy = pltpu.make_async_copy(tr_buf.at[t], tr_hbm.at[t], sem.at[t])
        copy.start()
        copies.append(copy)
    warm_buf[...] = warm[...] + corr[tracers + 1 : tracers + 2, :][None]
    copy = pltpu.make_async_copy(warm_buf, warm_hbm, sem.at[tracers + 2])
    copy.start()
    copies.append(copy)
    for copy in copies:
        copy.wait()


def local(nx, ny, q, u, v, w, d, level, a, b):
    tracers, rows, layers, lanes = q.shape
    tall = layers + 2 * PAD
    plane = (rows, layers, lanes)
    sum_rows = -(-(tracers + 2) // 8) * 8
    vmem = pltpu.VMEM
    dma = pltpu.SemaphoreType.DMA
    anywhere = pl.BlockSpec(memory_space=pl.ANY)
    inside = pl.BlockSpec(memory_space=vmem)
    middle = pl.pallas_call(
        functools.partial(main_kernel, nx, ny),
        name="remap_main",
        out_shape=[
            vmem((tracers,) + plane, F32),
            vmem(plane, F32),
            vmem(plane, F32),
            vmem(plane, F32),
            vmem((sum_rows, lanes), F32),
        ],
        in_specs=[anywhere] * 8,
        out_specs=[inside] * 5,
        scratch_shapes=[
            vmem((tracers,) + plane, jnp.bfloat16),
            vmem(plane, jnp.bfloat16),
            vmem(plane, jnp.bfloat16),
            vmem(plane, jnp.int32),
            vmem((tracers, rows, tall, lanes), F32),
            vmem((rows, tall, lanes), F32),
            vmem((rows, tall, lanes), F32),
            vmem((rows, tall, lanes), F32),
            vmem((tall, lanes), F32),
            vmem((rows, tall, lanes), F32),
            vmem((rows, tall, lanes), F32),
            vmem(plane, F32),
            vmem(plane, F32),
            vmem(plane, F32),
            vmem((layers, lanes), F32),
            vmem((tall, lanes), F32),
            vmem((layers, lanes), jnp.int32),
            vmem((layers, lanes), F32),
            vmem((layers, lanes), F32),
            vmem((tall, lanes), F32),
            vmem((sum_rows, lanes), F32),
            vmem((1, lanes), F32),
            vmem((1, lanes), F32),
            vmem((nx - 1, 1, lanes), F32),
            vmem((ny - 1, 1, lanes), F32),
            dma((8,)),
            dma((5,)),
            dma((5,)),
            dma((nx - 1,)),
            dma((nx - 1,)),
            dma((ny - 1,)),
            dma((ny - 1,)),
        ],
        compiler_params=pltpu.CompilerParams(collective_id=0, has_side_effects=True),
    )(q, u, v, w, d, level, a, b)
    return tuple(
        pl.pallas_call(
            finish_kernel,
            name="remap_finish",
            out_shape=[
                jax.ShapeDtypeStruct((tracers,) + plane, F32),
                jax.ShapeDtypeStruct(plane, F32),
                jax.ShapeDtypeStruct(plane, F32),
                jax.ShapeDtypeStruct(plane, F32),
            ],
            in_specs=[inside] * 5,
            out_specs=[anywhere] * 4,
            scratch_shapes=[
                vmem((tracers,) + plane, F32),
                vmem(plane, F32),
                dma((tracers + 3,)),
            ],
        )(*[pltpu.with_memory_space_constraint(x, vmem) for x in middle])
    )


def solution(mesh):
    flat = P("gy", None, "gx")
    tall = P(None, "gy", None, "gx")
    return jax.shard_map(
        functools.partial(local, mesh.shape["gx"], mesh.shape["gy"]),
        mesh=mesh,
        in_specs=(tall,) + (flat,) * 7,
        out_specs=(tall,) + (flat,) * 3,
        check_vma=False,
    )
```

```python
import functools

import jax
import jax.numpy as jnp
from jax import lax
from jax.experimental import pallas as pl
from jax.experimental.pallas import tpu as pltpu
from jax.sharding import PartitionSpec as P

MESH = pl.DeviceIdType.MESH
HEAT = 3.5
PAD = 8
DIRECT = 64
EARLY = 0
HELLOS = 4
F32 = jnp.float32
OFFSETS = (-2, -1, 0, 1, 2)


def choose(masks, options):
    keys = sorted(options)
    if len(keys) == len(OFFSETS):
        value = options[keys[-1]]
        keys = keys[:-1]
    else:
        value = jnp.zeros_like(options[keys[0]])
    for o in keys:
        value = jnp.where(masks[o], options[o], value)
    return value


def build_weights(depth_at, level, start, end, first_layer):
    layer = lax.broadcasted_iota(jnp.int32, level.shape, 0) + first_layer
    offset = level - layer
    masks = {o: offset == o for o in OFFSETS}
    depths = {o: depth_at(o) for o in range(-2, 4)}
    weight_first = (1.0 - start) * choose(masks, {o: depths[o] for o in OFFSETS})
    weight_second = end * choose(masks, {o: depths[o + 1] for o in OFFSETS})
    thick = weight_first + weight_second
    inverse = 1.0 / thick
    g1 = weight_first * inverse
    g2 = weight_second * inverse
    lin1 = 0.5 * (start + 1.0)
    sq1 = lin1 - (start * start + start + 1.0) * (1.0 / 3.0)
    lin2 = 0.5 * end
    sq2 = lin2 - end * end * (1.0 / 3.0)
    c_e0 = g1 * (1.0 - lin1 - 3.0 * sq1) * (1.0 / 12.0)
    c_e1 = (g1 * (lin1 - 3.0 * sq1) + g2 * (1.0 - lin2 - 3.0 * sq2)) * (1.0 / 12.0)
    c_e2 = g2 * (lin2 - 3.0 * sq2) * (1.0 / 12.0)
    taps = {
        -2: -c_e0,
        -1: 7.0 * c_e0 - c_e1,
        0: 7.0 * (c_e0 + c_e1) - c_e2 + 6.0 * (g1 * sq1),
        1: 7.0 * (c_e1 + c_e2) - c_e0 + 6.0 * (g2 * sq2),
        2: 7.0 * c_e2 - c_e1,
        3: -c_e2,
    }
    weights = {}
    for j in range(-4, 6):
        weights[j] = choose(masks, {o: taps[j - o] for o in OFFSETS if -2 <= j - o <= 3})
    return weights, thick


def remap(weights, load):
    terms = [weights[j] * load(j) for j in range(-4, 6)]
    while len(terms) > 1:
        terms = [
            terms[i] + terms[i + 1] if i + 1 < len(terms) else terms[i]
            for i in range(0, len(terms), 2)
        ]
    return terms[0]


def ghosts(near, second, third):
    return near + second - third, 12.0 * second - 4.0 * near - 7.0 * third


def pad_ends(buf, layers):
    row = lax.broadcasted_iota(jnp.int32, (PAD, buf.shape[-1]), 0)
    one, two = ghosts(
        buf[PAD : PAD + 1, :], buf[PAD + 1 : PAD + 2, :], buf[PAD + 2 : PAD + 3, :]
    )
    buf[0:PAD, :] = jnp.where(row == PAD - 1, one, jnp.where(row == PAD - 2, two, 0.0))
    last = PAD + layers
    one, two = ghosts(
        buf[last - 1 : last, :], buf[last - 2 : last - 1, :], buf[last - 3 : last - 2, :]
    )
    buf[last : last + PAD, :] = jnp.where(row == 0, one, jnp.where(row == 1, two, 0.0))


def one_step(nx, ny):
    return nx * ny <= DIRECT


def greeting_rounds(nx, ny):
    def around(steps):
        return sorted({(x % nx, y % ny) for x, y in steps} - {(0, 0)})

    first = around([(1, 0), (-1, 0), (0, 1), (0, -1)])
    known = {(0, 0)} | set(first)
    rounds = []
    while len(known) < nx * ny:
        told = first
        if rounds:
            told = [p for p in around([(2, 0), (-2, 0), (0, 2), (0, -2)]) if p in known]
        more = {((p[0] + x) % nx, (p[1] + y) % ny) for p in told for x, y in known} | known
        slim_told = [p for p in told if p[0] == 0]
        slim = {((p[0] + x) % nx, (p[1] + y) % ny) for p in slim_told for x, y in known} | known
        if len(slim) == nx * ny:
            told, more = slim_told, slim
        if len(more) == len(known):
            return None, None
        rounds.append(told)
        known = more
    return first, rounds


def main_kernel(
    nx,
    ny,
    q_hbm,
    u_hbm,
    v_hbm,
    w_hbm,
    d_hbm,
    l_hbm,
    a_hbm,
    b_hbm,
    tr_out,
    zonal_out,
    merid_out,
    warm_out,
    corr_out,
    q_raw,
    a_raw,
    b_raw,
    level,
    q_pad,
    u_pad,
    v_pad,
    vr_pad,
    vb_pad,
    w_pad,
    d_pad,
    a32,
    b32,
    thick_all,
    packed,
    n_depth,
    n_level,
    n_start,
    n_end,
    e_packed,
    sums,
    mine_x,
    mine_y,
    got_x,
    got_y,
    in_sem,
    send_sem,
    recv_sem,
    x_sem,
    y_sem,
    hello,
):
    tracers, rows, layers, lanes = q_raw.shape
    gx = lax.axis_index("gx")
    gy = lax.axis_index("gy")
    body = pl.ds(PAD, layers)

    def x_peer(k):
        return {"gx": lax.rem(gx + k, nx)}

    def y_peer(k):
        return {"gy": lax.rem(gy + k, ny)}

    def at_steps(p):
        place = {}
        if p[0]:
            place.update(x_peer(p[0]))
        if p[1]:
            place.update(y_peer(p[1]))
        return place

    def greet(n):
        if n < len(rounds):
            for p in rounds[n]:
                pl.semaphore_signal(
                    hello.at[n], inc=1, device_id=at_steps(p), device_id_type=MESH
                )

    def hear(n):
        if 0 <= n < len(rounds):
            pl.semaphore_wait(hello.at[n], len(rounds[n]))

    def peer_groups():
        along_x = [x_peer(k) for k in range(1, nx)]
        along_y = [y_peer(k) for k in range(1, ny)]
        if not one_step(nx, ny):
            return [along_x, along_y]
        both = [{**x, **y} for x in along_x for y in along_y]
        return [both + along_y + along_x]

    loads = [
        pltpu.make_async_copy(a_hbm, a_raw, in_sem.at[0]),
        pltpu.make_async_copy(b_hbm, b_raw, in_sem.at[1]),
        pltpu.make_async_copy(l_hbm, level, in_sem.at[2]),
        pltpu.make_async_copy(d_hbm, d_pad.at[:, body, :], in_sem.at[3]),
        pltpu.make_async_copy(v_hbm, v_pad.at[:, body, :], in_sem.at[4]),
        pltpu.make_async_copy(u_hbm, u_pad.at[:, body, :], in_sem.at[5]),
        pltpu.make_async_copy(w_hbm, w_pad.at[:, body, :], in_sem.at[6]),
        pltpu.make_async_copy(q_hbm, q_raw, in_sem.at[7]),
    ]
    for load in loads:
        load.start()

    barrier = pltpu.get_barrier_semaphore()
    first_met, rounds = greeting_rounds(nx, ny) if one_step(nx, ny) else (None, None)
    if rounds is None:
        greeted = [peer for group in peer_groups() for peer in group]
        rounds = []
    else:
        greeted = [at_steps(p) for p in first_met]
    for peer in greeted:
        pl.semaphore_signal(barrier, inc=1, device_id=peer, device_id_type=MESH)

    for load in loads[:4]:
        load.wait()
    lane_full = lax.broadcasted_iota(jnp.int32, (layers, lanes), 1)
    for r in range(rows):
        a32[r] = a_raw[r].astype(F32)
        b32[r] = b_raw[r].astype(F32)
    column = jnp.zeros((layers, lanes), F32)
    for r in range(rows):
        parts = (d_pad[r, PAD : PAD + layers, :], level[r].astype(F32), a32[r], b32[r])
        for q, part in enumerate(parts):
            spot = q * rows + r
            moved = pltpu.roll(part, spot, 1) if spot else part
            column = jnp.where(lane_full == spot, moved, column)
    packed[...] = column

    for load in loads[4:7]:
        load.wait()
    for r in range(rows):
        d_pad[r, 0:PAD, :] = jnp.zeros((PAD, lanes), F32)
        d_pad[r, PAD + layers : PAD + layers + PAD, :] = jnp.zeros((PAD, lanes), F32)
        pad_ends(v_pad.at[r], layers)
        pad_ends(u_pad.at[r], layers)
        pad_ends(w_pad.at[r], layers)
    lane_tall = lax.broadcasted_iota(jnp.int32, (layers + 2 * PAD, lanes), 1)
    last_faces = jnp.zeros((layers + 2 * PAD, lanes), F32)
    for r in range(rows):
        wind = v_pad[r]
        turned = pltpu.roll(wind, 1, 1)
        vr_pad[r] = turned
        moved = pltpu.roll(turned, r, 1) if r else turned
        last_faces = jnp.where(lane_tall == r, moved, last_faces)
    vb_pad[...] = last_faces
    loads[7].wait()
    for t in range(tracers):
        for r in range(rows):
            q_pad[t, r, PAD : PAD + layers, :] = q_raw[t, r].astype(F32)
            pad_ends(q_pad.at[t, r], layers)

    lane = lax.broadcasted_iota(jnp.int32, (8, lanes), 1)
    not_first = lane > 0
    not_last = lane < lanes - 1
    zero = jnp.zeros((8, lanes), F32)

    def tile_step(i, carry):
        masses, total, energy = carry
        masses = list(masses)
        k0 = pl.multiple_of(i * 8, 8)
        here = pl.ds(k0, 8)

        def at(ref, j):
            return ref[pl.ds(k0 + (PAD + j), 8), :]

        own_before = None
        thick_before = None
        for r in range(rows):
            weights, thick = build_weights(
                lambda o: at(d_pad.at[r], o), level[r, here, :], a32[r, here, :], b32[r, here, :], k0
            )
            depth = at(d_pad.at[r], 0)
            thick_all[r, here, :] = thick
            total = total + thick
            for t in range(tracers):
                new = remap(weights, lambda j: at(q_pad.at[t, r], j))
                tr_out[t, r, here, :] = new
                masses[t] = masses[t] + (depth * at(q_pad.at[t, r], 0) - thick * new)
            warm = remap(weights, lambda j: at(w_pad.at[r], j))
            warm_out[r, here, :] = warm
            energy = energy + HEAT * (depth * at(w_pad.at[r], 0) - thick * warm)
            u_here = at(u_pad.at[r], 0)
            squares = u_here * u_here
            own = remap(weights, lambda j: at(u_pad.at[r], j))
            after = zero
            if r > 0:
                u_back = at(u_pad.at[r - 1], 0)
                squares = squares + u_back * u_back
                cross = remap(weights, lambda j: at(u_pad.at[r - 1], j))
                zonal = 0.5 * (own_before + cross)
                zonal_out[r - 1, here, :] = zonal
                after = (thick_before + thick) * (zonal * zonal)
            own_before = own
            thick_before = thick
            v_here = at(v_pad.at[r], 0)
            v_west = at(vr_pad.at[r], 0)
            squares = squares + v_here * v_here + jnp.where(not_first, v_west * v_west, 0.0)
            own_v = remap(weights, lambda j: at(v_pad.at[r], j))
            cross_v = remap(weights, lambda j: at(vr_pad.at[r], j))
            east_v = jnp.where(not_last, pltpu.roll(cross_v, lanes - 1, 1), 0.0)
            east_thick = pltpu.roll(thick, lanes - 1, 1)
            merid = 0.5 * (own_v + east_v)
            merid_out[r, here, :] = merid
            after = after + jnp.where(not_last, (thick + east_thick) * (merid * merid), 0.0)
            energy = energy + 0.25 * (depth * squares - after)
        zonal_out[rows - 1, here, :] = own_before
        return tuple(masses), total, energy

    tiles = layers // 8
    early = min(EARLY, tiles)
    carry = lax.fori_loop(0, early, tile_step, ((zero,) * tracers, zero, zero))
    pl.semaphore_wait(barrier, len(greeted))
    pairs = [
        (packed, e_packed.at[body, :], x_peer(nx - 1)),
        (d_pad.at[0, body, :], n_depth.at[body, :], y_peer(ny - 1)),
        (level.at[0], n_level, y_peer(ny - 1)),
        (a32.at[0], n_start, y_peer(ny - 1)),
        (b32.at[0], n_end, y_peer(ny - 1)),
    ]
    sends = [
        pltpu.make_async_remote_copy(
            src_ref=src,
            dst_ref=dst,
            send_sem=send_sem.at[i],
            recv_sem=recv_sem.at[i],
            device_id=peer,
            device_id_type=MESH,
        )
        for i, (src, dst, peer) in enumerate(pairs)
    ]
    for send in sends:
        send.start()

    greet(0)
    pieces = max(len(rounds), 1)
    marks = [early + (tiles - early) * n // pieces for n in range(pieces + 1)]
    for n in range(pieces):
        carry = lax.fori_loop(marks[n], marks[n + 1], tile_step, carry)
        if n + 1 < pieces:
            hear(n)
            greet(n + 1)
    masses, total, energy = carry
    sums[...] = jnp.zeros(sums.shape, F32)
    for t in range(tracers):
        sums[t : t + 1, :] = jnp.sum(masses[t], axis=0, keepdims=True)
    sums[tracers : tracers + 1, :] = jnp.sum(total, axis=0, keepdims=True)

    for send in sends:
        send.wait_recv()

    def edge_step(i, energy):
        k0 = pl.multiple_of(i * 8, 8)
        here = pl.ds(k0, 8)

        def at(ref, j):
            return ref[pl.ds(k0 + (PAD + j), 8), :]

        weights, thick = build_weights(
            lambda o: at(n_depth, o), n_level[here, :], n_start[here, :], n_end[here, :], k0
        )
        u_last = at(u_pad.at[rows - 1], 0)
        cross = remap(weights, lambda j: at(u_pad.at[rows - 1], j))
        zonal = 0.5 * (zonal_out[rows - 1, here, :] + cross)
        zonal_out[rows - 1, here, :] = zonal
        change = at(n_depth, 0) * (u_last * u_last) - (
            thick_all[rows - 1, here, :] + thick
        ) * (zonal * zonal)

        column = at(e_packed, 0)
        weights, thick = build_weights(
            lambda o: at(e_packed, o),
            pltpu.roll(column, lanes - rows, 1).astype(jnp.int32),
            pltpu.roll(column, lanes - 2 * rows, 1),
            pltpu.roll(column, lanes - 3 * rows, 1),
            k0,
        )
        cross = remap(weights, lambda j: at(vb_pad, j))
        face = at(vb_pad, 0)
        change = change + jnp.where(lane < rows, column * (face * face), 0.0)
        for r in range(rows):
            there = pltpu.roll(cross, lanes - 1 - r, 1)
            there_thick = pltpu.roll(thick, lanes - 1 - r, 1)
            merid = merid_out[r, here, :] + jnp.where(not_last, 0.0, 0.5 * there)
            merid_out[r, here, :] = merid
            change = change - jnp.where(
                not_last, 0.0, (thick_all[r, here, :] + there_thick) * (merid * merid)
            )
        return energy + 0.25 * change

    energy = lax.fori_loop(0, layers // 8, edge_step, energy)
    sums[tracers + 1 : tracers + 2, :] = jnp.sum(energy, axis=0, keepdims=True)

    wide = sums.shape
    diagonal = lax.broadcasted_iota(jnp.int32, wide, 0) == lax.broadcasted_iota(jnp.int32, wide, 1)
    column = jnp.sum(sums[...], axis=1, keepdims=True)
    mine_x[...] = jnp.sum(jnp.where(diagonal, column, 0.0), axis=0, keepdims=True)

    def gather(peers, mine, got, sems):
        copies = [
            pltpu.make_async_remote_copy(
                src_ref=mine,
                dst_ref=got.at[k],
                send_sem=sems.at[0],
                recv_sem=sems.at[1],
                device_id=peer,
                device_id_type=MESH,
            )
            for k, peer in enumerate(peers)
        ]
        for copy in copies:
            copy.start()
        everything = pltpu.make_async_remote_copy(
            src_ref=got,
            dst_ref=got,
            send_sem=sems.at[0],
            recv_sem=sems.at[1],
            device_id=peers[0],
            device_id_type=MESH,
        )
        everything.wait_recv()
        value = mine[...] + jnp.sum(got[...], axis=0)
        return value, everything

    hear(len(rounds) - 1)
    groups = peer_groups()
    value, first = gather(groups[0], mine_x, got_x, x_sem)
    ends = [first]
    if len(groups) > 1:
        mine_y[...] = value
        value, second = gather(groups[1], mine_y, got_y, y_sem)
        ends.append(second)

    spread = jnp.sum(jnp.where(diagonal, value, 0.0), axis=1, keepdims=True)
    total_new = spread[tracers : tracers + 1, :]
    change = spread / total_new
    index = lax.broadcasted_iota(jnp.int32, change.shape, 0)
    change = jnp.where(index == tracers + 1, change * (1.0 / HEAT), change)
    corr_out[...] = jnp.broadcast_to(change, corr_out.shape)
    for send in sends:
        send.wait_send()
    for end in ends:
        end.wait_send()


def finish_kernel(
    tr,
    zonal,
    merid,
    warm,
    corr,
    tr_hbm,
    zonal_hbm,
    merid_hbm,
    warm_hbm,
    tr_buf,
    warm_buf,
    sem,
):
    tracers = tr.shape[0]
    copies = [
        pltpu.make_async_copy(zonal, zonal_hbm, sem.at[tracers]),
        pltpu.make_async_copy(merid, merid_hbm, sem.at[tracers + 1]),
    ]
    for copy in copies:
        copy.start()
    for t in range(tracers):
        tr_buf[t] = tr[t] + corr[t : t + 1, :][None]
        copy = pltpu.make_async_copy(tr_buf.at[t], tr_hbm.at[t], sem.at[t])
        copy.start()
        copies.append(copy)
    warm_buf[...] = warm[...] + corr[tracers + 1 : tracers + 2, :][None]
    copy = pltpu.make_async_copy(warm_buf, warm_hbm, sem.at[tracers + 2])
    copy.start()
    copies.append(copy)
    for copy in copies:
        copy.wait()


def local(nx, ny, q, u, v, w, d, level, a, b):
    tracers, rows, layers, lanes = q.shape
    tall = layers + 2 * PAD
    plane = (rows, layers, lanes)
    sum_rows = -(-(tracers + 2) // 8) * 8
    vmem = pltpu.VMEM
    dma = pltpu.SemaphoreType.DMA
    anywhere = pl.BlockSpec(memory_space=pl.ANY)
    inside = pl.BlockSpec(memory_space=vmem)
    middle = pl.pallas_call(
        functools.partial(main_kernel, nx, ny),
        name="remap_main",
        out_shape=[
            vmem((tracers,) + plane, F32),
            vmem(plane, F32),
            vmem(plane, F32),
            vmem(plane, F32),
            vmem((sum_rows, lanes), F32),
        ],
        in_specs=[anywhere] * 8,
        out_specs=[inside] * 5,
        scratch_shapes=[
            vmem((tracers,) + plane, jnp.bfloat16),
            vmem(plane, jnp.bfloat16),
            vmem(plane, jnp.bfloat16),
            vmem(plane, jnp.int32),
            vmem((tracers, rows, tall, lanes), F32),
            vmem((rows, tall, lanes), F32),
            vmem((rows, tall, lanes), F32),
            vmem((rows, tall, lanes), F32),
            vmem((tall, lanes), F32),
            vmem((rows, tall, lanes), F32),
            vmem((rows, tall, lanes), F32),
            vmem(plane, F32),
            vmem(plane, F32),
            vmem(plane, F32),
            vmem((layers, lanes), F32),
            vmem((tall, lanes), F32),
            vmem((layers, lanes), jnp.int32),
            vmem((layers, lanes), F32),
            vmem((layers, lanes), F32),
            vmem((tall, lanes), F32),
            vmem((sum_rows, lanes), F32),
            vmem((1, lanes), F32),
            vmem((1, lanes), F32),
            vmem((nx * ny - 1 if one_step(nx, ny) else nx - 1, 1, lanes), F32),
            vmem((ny - 1, 1, lanes), F32),
            dma((8,)),
            dma((5,)),
            dma((5,)),
            dma((2,)),
            dma((2,)),
            pltpu.SemaphoreType.REGULAR((HELLOS,)),
        ],
        compiler_params=pltpu.CompilerParams(collective_id=0, has_side_effects=True),
    )(q, u, v, w, d, level, a, b)
    return tuple(
        pl.pallas_call(
            finish_kernel,
            name="remap_finish",
            out_shape=[
                jax.ShapeDtypeStruct((tracers,) + plane, F32),
                jax.ShapeDtypeStruct(plane, F32),
                jax.ShapeDtypeStruct(plane, F32),
                jax.ShapeDtypeStruct(plane, F32),
            ],
            in_specs=[inside] * 5,
            out_specs=[anywhere] * 4,
            scratch_shapes=[
                vmem((tracers,) + plane, F32),
                vmem(plane, F32),
                dma((tracers + 3,)),
            ],
        )(*[pltpu.with_memory_space_constraint(x, vmem) for x in middle])
    )


def solution(mesh):
    flat = P("gy", None, "gx")
    tall = P(None, "gy", None, "gx")
    return jax.shard_map(
        functools.partial(local, mesh.shape["gx"], mesh.shape["gy"]),
        mesh=mesh,
        in_specs=(tall,) + (flat,) * 7,
        out_specs=(tall,) + (flat,) * 3,
        check_vma=False,
    )
```
